128 devices in a mesh: node: 16 (over z, y), dev: 8 (over x, core).
Axes of the slice: x: 4, y: 4, z: 4, core: 2. Of those that a mesh axis runs over, the one named last changes fastest.
Arguments:
- tokens: bfloat16 [8192, 5120], P(('node', 'dev')), may hold values from -6 to 6
- node_ids: int32 [8192, 3], P(('node', 'dev')), may hold values from 0 to 15, all different within a row; in each aligned block of 64 rows (0 to 63, 64 to 127, ...) at most 13 rows name the same one
- expert_pick: int32 [8192, 6], P(('node', 'dev')), may hold values from 0 to 8, all different within a row
- gate_share: bfloat16 [8192, 6], P(('node', 'dev')), may hold values from 0.099609375 to 1
- gate_proj: bfloat16 [48, 1536, 5120], P('node', 'dev'), may hold values from -0.078125 to 0.078125
- up_proj: bfloat16 [48, 1536, 5120], P('node', 'dev'), may hold values from -0.078125 to 0.078125
- down_proj: bfloat16 [48, 1536, 5120], P('node', 'dev'), may hold values from -0.15625 to 0.15625
Outputs:
- moe_out: bfloat16 [8192, 5120], P(('node', 'dev'))
The draws below stay inside these ranges and needn't reach their ends.
Inputs may be any that keep to these rules, and one draw needn't show every extreme that they name: `node_ids`: A token names 3 different groups; at most 13 tokens of one device name one group, and some device reaches 13 in every draw. `expert_pick`: A token names 6 different picks; pick p selects local expert p % 3 of the token's group choice p // 3.
All inputs are finite; a program needn't handle non-finite values.
Results may differ from the reference program's by a relative error of at most 0.0085.
Values may be sent and summed in bfloat16 or wider, within the bound.
A program may use at most 256 MiB of HBM per device.

```python
import math
import jax
import jax.numpy as jnp
import numpy as np
from jax import lax

D = 5120
FF = 1536
TOP = 6
TOP_NODES = 3
EXP_NODE = 3
TOK_DEV = 64
EXPERTS = 48
CAP = 13
TOKENS = 8192
N_NODE = 16
N_DEV = 8


def level_of(rng, extent, pieces, least, largest):
    def one(axis_at, shards_of):
        steps = jax.random.uniform(jax.random.fold_in(jax.random.fold_in(rng, 6), axis_at), (shards_of,), jnp.float32, least / len(pieces), largest / len(pieces))
        return jnp.repeat(jnp.exp(steps), extent[axis_at] // shards_of).reshape((-1,) + (1,) * (len(extent) - axis_at - 1))

    gain = one(*pieces[0])
    for cut in pieces[1:]:
        gain = gain * one(*cut)
    return gain


def different_ones(own_key, rows, count, top, lift):
    order = jax.random.permutation(jax.random.fold_in(own_key, 1), count)
    pull = order
    for power in range(3):
        pull = pull * pull // count
    pull = pull * lift // count
    lots = jax.random.randint(jax.random.fold_in(own_key, 2), (rows, count), 0, 4096) + pull
    fixed_rows = jax.random.permutation(jax.random.fold_in(own_key, 3), rows)[jnp.arange(count) % rows]
    lots = jnp.where(jnp.arange(rows)[:, None] == fixed_rows[None, :], 1 << 14, lots)
    merit = lots * count + jnp.arange(count)
    return lax.top_k(merit.astype(jnp.int32), top)[1].astype(jnp.int32)


def deal_out(rng, own, number, rows, count, top, bound, lean):
    sequence = jax.random.permutation(rng, count)
    packed, common = portions_of(count, rows * top, bound, lean, True), portions_of(count, rows * top, bound, lean, False)
    places = jnp.arange(count)

    def named(lengths, offset_by):
        used = int((lengths > 0).sum())
        fixed = max(1, used // 4)
        passed = fixed + (places - fixed + offset_by * (used - fixed)) % max(1, count - fixed)
        return jnp.zeros((count,), jnp.int32).at[sequence[jnp.where(places < fixed, places, passed)]].set(jnp.asarray(lengths, jnp.int32))

    lengths = jnp.where(number % 4 == 0, named(packed, number // 4), named(common, number - number // 4 - 1))
    mixed = jax.random.permutation(jax.random.fold_in(own, 3), count)
    donor, receiver = mixed[0:count // 2 * 2:2], mixed[1:count // 2 * 2:2]
    slack = jnp.minimum(lengths[donor] - 1, bound - lengths[receiver]) // 2
    slack = jnp.where((donor == sequence[0]) | (receiver == sequence[0]) | (lengths[receiver] == 0), 0, jnp.maximum(slack, 0))
    passed = jax.random.randint(jax.random.fold_in(own, 4), (count // 2,), 0, 1 << 20) % (slack + 1)
    lengths = lengths.at[donor].add(-passed).at[receiver].add(passed)
    members = jnp.searchsorted(jnp.cumsum(lengths), jnp.arange(rows * top), side="right").astype(jnp.int32)
    table = members.reshape(top, rows).T
    table = table[jax.random.permutation(jax.random.fold_in(own, 1), rows)]
    offset_by = jax.random.randint(jax.random.fold_in(own, 2), (rows, 1), 0, top)
    return jnp.take_along_axis(table, (jnp.arange(top)[None, :] + offset_by) % top, axis=1)


def portions_of(count, total, bound, slope, full):
    loads = [(1 << 20) // math.isqrt(grade ** slope) + 1 for grade in range(1, count + 1)]
    largest = bound if full else min(bound, max(-(-total // count), total * loads[0] // sum(loads)))
    least = 1 if total - largest >= count - 1 else 0
    given, surplus = [largest] + [least] * (count - 1), total - largest - least * (count - 1)
    while surplus > 0:
        free = [i for i in range(1, count) if given[i] < largest] or [i for i in range(1, count) if given[i] < bound]
        whole, left = sum([loads[i] for i in free]), surplus
        for i in free:
            extra = min(bound - given[i], max(1, left * loads[i] // whole), surplus)
            given[i] = given[i] + extra
            surplus = surplus - extra
    return np.array(given)


def noise(key, dims, spread, bound, cuts=(), kind=jnp.bfloat16):
    drawn = jax.random.normal(key, dims, jnp.float32) * spread
    if len(cuts) > 0:
        drawn = level_of(key, dims, cuts, -0.22, 0.18) * drawn
    return jnp.clip(drawn, min=-bound, max=bound).astype(kind)


def setup_inputs(seed: int = 0) -> dict:
    streams_of = jax.random.split(jax.random.key(seed), 8)
    tokens = noise(streams_of[0], (TOKENS, D), 1.0, 6.0, ((0, 128),))
    node_ids_keys = jax.random.split(jax.random.fold_in(streams_of[1], 1), TOKENS // TOK_DEV)
    node_ids_turns = jax.random.permutation(jax.random.fold_in(streams_of[1], 3), TOKENS // TOK_DEV)
    node_ids = jax.vmap(lambda own, number: deal_out(jax.random.fold_in(streams_of[1], 2), own, number, TOK_DEV, N_NODE, TOP_NODES, CAP, 2))(node_ids_keys, node_ids_turns).reshape((TOKENS, TOP_NODES))
    expert_pick = different_ones(streams_of[2], TOKENS, TOP_NODES * EXP_NODE, TOP, 0)
    gate_share = jnp.clip(jnp.exp(math.log(1.0) - 2.306499 * jax.random.uniform(streams_of[3], (TOKENS, TOP), jnp.float32) ** level_of(streams_of[3], (TOKENS, TOP), ((0, 128),), -0.2, 0.2)), 0.099609375, 1.0).astype(jnp.bfloat16)
    gate_proj = noise(streams_of[4], (EXPERTS, FF, D), D ** -0.5, 0.078125, ((0, 16), (1, 8)))
    up_proj = noise(streams_of[5], (EXPERTS, FF, D), D ** -0.5, 0.078125, ((0, 16), (1, 8)))
    down_proj = noise(streams_of[6], (EXPERTS, FF, D), FF ** -0.5, 0.15625, ((0, 16), (1, 8)))
    return {"tokens": tokens, "node_ids": node_ids, "expert_pick": expert_pick, "gate_share": gate_share, "gate_proj": gate_proj, "up_proj": up_proj, "down_proj": down_proj}


def reference(tokens, node_ids, expert_pick, gate_share, gate_proj, up_proj, down_proj):
    token_count = tokens.shape[0]
    capacity = CAP * N_NODE * N_DEV
    candidates = TOP_NODES * EXP_NODE
    slice_width = FF // N_DEV
    picked = (expert_pick[:, :, None] == jnp.arange(candidates, dtype=jnp.int32)[None, None, :]).astype(jnp.float32)
    shares = jnp.einsum('tj,tjq->tq', gate_share.astype(jnp.float32), picked, precision=lax.Precision.HIGHEST)
    shares = shares.reshape(token_count, TOP_NODES, EXP_NODE)
    contract = (((1,), (1,)), ((), ()))

    def per_node(total, node_index):
        hit_mask = (node_ids == node_index).astype(jnp.int32)
        chosen = jnp.sum(hit_mask, axis=1) > 0
        positions = jnp.nonzero(chosen, size=capacity, fill_value=0)[0].astype(jnp.int32)
        is_valid = (jnp.arange(capacity, dtype=jnp.int32) < jnp.sum(chosen.astype(jnp.int32))).astype(jnp.float32)
        node_shares = jnp.einsum('tk,tke->te', hit_mask.astype(jnp.float32), shares, precision=lax.Precision.HIGHEST)
        node_shares = node_shares[positions] * is_valid[:, None]
        tok_rows = tokens[positions]
        accumulated = jnp.zeros((capacity, N_DEV, D), jnp.float32)
        for expert_local in range(EXP_NODE):
            expert = (node_index * EXP_NODE + expert_local).astype(jnp.int32)
            w_gate = lax.dynamic_index_in_dim(gate_proj, expert, 0, keepdims=False)
            w_up = lax.dynamic_index_in_dim(up_proj, expert, 0, keepdims=False)
            w_down = lax.dynamic_index_in_dim(down_proj, expert, 0, keepdims=False)
            gate_val = lax.dot_general(tok_rows, w_gate, contract, preferred_element_type=jnp.float32)
            up_val = lax.dot_general(tok_rows, w_up, contract, preferred_element_type=jnp.float32)
            hidden = (jax.nn.silu(gate_val) * up_val).astype(jnp.bfloat16)
            grouped = jnp.einsum('rgf,gfd->rgd', hidden.reshape(capacity, N_DEV, slice_width).astype(jnp.float32),
                                 w_down.reshape(N_DEV, slice_width, D).astype(jnp.float32),
                                 precision=lax.Precision.HIGHEST)
            accumulated = accumulated + node_shares[:, expert_local, None, None] * grouped
        partial_value = lax.optimization_barrier(accumulated.astype(jnp.bfloat16)).astype(jnp.float32)
        contrib = jnp.sum(partial_value, axis=1) * is_valid[:, None]
        return total.at[positions].add(contrib), None

    total, _ = lax.scan(per_node, jnp.zeros((token_count, D), jnp.float32), jnp.arange(N_NODE, dtype=jnp.int32))
    return total.astype(jnp.bfloat16)
```

```python
import functools
import math

import jax
import jax.numpy as jnp
from jax import lax
from jax.experimental import pallas as pl
from jax.experimental.pallas import tpu as pltpu
from jax.sharding import PartitionSpec as P

LANES = 128
SLOTS = 16
CAP = 13
BLOCK = 64
F32 = jnp.float32
BF16 = jnp.bfloat16
MESH = pl.DeviceIdType.MESH
CUTS = (0, 48, 96, 160, 208)
HOPS = (
    (0, 0), (0, 1), (1, 0), (0, 3), (3, 0), (1, 1), (1, 2), (2, 1),
    (2, 2), (2, 3), (3, 2), (0, 2), (2, 0), (1, 3), (3, 1), (3, 3),
)


def kernel(
    send_ref, gate_ref, up_ref, down_ref, back_ref,
    wgu, wd, xbuf, exr, pr, ra, rb, fl, fr, hbuf,
    wsem, exs, exv, ags, agv, rss, rsv, rts, rtv,
):
    local, hidden, width = gate_ref.shape
    nodes = len(HOPS)
    side = math.isqrt(nodes)
    half = width // 2
    tiles = wgu.shape[0]
    node = lax.axis_index("node")
    dev = lax.axis_index("dev")
    z, y = node // side, node % side
    ring = 4
    cx, core = dev // 2, dev % 2
    right = {"dev": (cx + 1) % ring * 2 + core}
    left = {"dev": (cx + ring - 1) % ring * 2 + core}
    partner = {"dev": cx * 2 + (1 - core)}

    def there(p):
        dz, dy = HOPS[p]
        return {"node": (z + dz) % side * side + (y + dy) % side}

    def back_there(p):
        dz, dy = HOPS[p]
        return {"node": (z + side - dz) % side * side + (y + side - dy) % side}

    def remote(src, dst, ssem, rsem, device):
        return pltpu.make_async_remote_copy(
            src_ref=src, dst_ref=dst, send_sem=ssem, recv_sem=rsem,
            device_id=device, device_id_type=MESH,
        )

    weights = []
    for e in range(local):
        for b in range(hidden // BLOCK):
            blk = e * (hidden // BLOCK) + b
            i, at = blk // 2, blk % 2 * BLOCK
            rows = pl.ds(b * BLOCK, BLOCK)
            weights.append((gate_ref.at[e, rows], wgu.at[i, pl.ds(at, BLOCK)]))
            weights.append((up_ref.at[e, rows], wgu.at[i, pl.ds(LANES + at, BLOCK)]))
        weights.append((down_ref.at[e], wd.at[pl.ds(e * hidden, hidden)]))
    weights = [
        pltpu.make_async_copy(s, d, wsem.at[i]) for i, (s, d) in enumerate(weights)
    ]

    barrier = pltpu.get_barrier_semaphore()
    for p in range(1, nodes):
        pl.semaphore_signal(barrier, inc=1, device_id=there(p), device_id_type=MESH)
    for device in (right, left, partner):
        pl.semaphore_signal(barrier, inc=1, device_id=device, device_id_type=MESH)
    own_in = pltpu.make_async_copy(send_ref.at[0], exr.at[pl.ds(0, SLOTS)], exs.at[0])
    own_in.start()
    for w in weights:
        w.start()
    used = local * hidden
    if used < tiles * LANES:
        rest = tiles * LANES - used
        wgu[tiles - 1, LANES - rest : LANES] = jnp.zeros((rest, width), BF16)
        wgu[tiles - 1, 2 * LANES - rest :] = jnp.zeros((rest, width), BF16)
        wd[used:] = jnp.zeros((rest, width), BF16)
    pl.semaphore_wait(barrier, nodes + 2)

    exchange = {}
    for p in range(1, nodes):
        exchange[p] = remote(
            send_ref.at[p], exr.at[pl.ds(p * SLOTS, SLOTS)], exs.at[p], exv.at[p], there(p)
        )
        exchange[p].start()

    chunks = list(zip(CUTS[:-1], CUTS[1:]))
    ag = [{} for _ in chunks]
    rs = [{} for _ in chunks]
    state = {"arrived": 0, "returned": 0}
    ret = {}

    def onehot(rows, cols, hit):
        i = lax.broadcasted_iota(jnp.int32, (rows, cols), 0)
        j = lax.broadcasted_iota(jnp.int32, (rows, cols), 1)
        return hit(i, j).astype(F32).astype(BF16)

    def own(c):
        a, b = chunks[c]
        n0, n1 = a // CAP, (b - 1) // CAP + 1
        while state["arrived"] < n1:
            p = state["arrived"]
            if p == 0:
                own_in.wait()
            else:
                exchange[p].wait_recv()
            state["arrived"] += 1
        def hit(i, j):
            match = None
            for p in range(n0, n1):
                k = j - (p - n0) * SLOTS
                m = (k >= 0) & (k < CAP) & (i + a == k + p * CAP)
                match = m if match is None else match | m
            return match

        pick = onehot(b - a, (n1 - n0) * SLOTS, hit)
        dense = jnp.dot(
            pick, exr[n0 * SLOTS : n1 * SLOTS, :], preferred_element_type=F32
        )
        xbuf[0, a:b, :] = dense.astype(BF16)
        rows = pl.ds(a, b - a)
        mine = xbuf.at[0, rows]
        ag[c][0] = remote(mine, xbuf.at[3, rows], ags.at[c, 0], agv.at[c, 0], right)
        ag[c][1] = remote(mine, xbuf.at[1, rows], ags.at[c, 1], agv.at[c, 1], left)
        ag[c][2] = remote(mine, xbuf.at[4, rows], ags.at[c, 2], agv.at[c, 2], partner)
        for q in range(3):
            ag[c][q].start()

    def relay(c):
        a, b = chunks[c]
        rows = pl.ds(a, b - a)
        low, high = pl.ds(0, half), pl.ds(half, xbuf.shape[2] - half)
        ag[c][3] = remote(
            xbuf.at[3, rows, low], xbuf.at[2, rows, low], ags.at[c, 3], agv.at[c, 3], right
        )
        ag[c][4] = remote(
            xbuf.at[1, rows, high], xbuf.at[2, rows, high], ags.at[c, 4], agv.at[c, 4], left
        )
        for q, s in ((5, 3), (6, 1), (7, 2)):
            ag[c][q] = remote(
                xbuf.at[s, rows], xbuf.at[4 + s, rows], ags.at[c, q], agv.at[c, q], partner
            )
        ag[c][0].wait_recv()
        ag[c][3].start()
        ag[c][5].start()
        ag[c][1].wait_recv()
        ag[c][4].start()
        ag[c][6].start()

    def far(c):
        ag[c][3].wait_recv()
        ag[c][4].wait_recv()
        ag[c][7].start()
        for q in (2, 5, 6, 7):
            ag[c][q].wait_recv()

    def compute(c):
        a, b = chunks[c]
        span = b - a
        count = 8 * span

        def hidden_tile(i, _):
            x = xbuf[:, a:b, :width].reshape(count, width)
            acc = lax.dot_general(
                x, wgu[i], (((1,), (1,)), ((), ())), preferred_element_type=F32
            )
            g, u = acc[:, :LANES], acc[:, LANES:]
            shares = xbuf[:, a:b, width:].reshape(count, LANES)

            def hit(e, j):
                at = j + i * LANES - e * hidden
                return (at >= 0) & (at < hidden) & (e < local)

            scale = jnp.dot(
                shares, onehot(LANES, LANES, hit), preferred_element_type=F32
            )
            h = g / (1.0 + jnp.exp(-g)) * u * scale
            hbuf[:count, pl.ds(pl.multiple_of(i * LANES, LANES), LANES)] = h.astype(BF16)
            return _

        lax.fori_loop(0, tiles, hidden_tile, 0)
        for q in range(8):
            ag[c][q].wait_send()

        tile = 512

        def down_tile(n, _):
            cols = pl.ds(pl.multiple_of(n * tile, tile), tile)
            out = jnp.dot(hbuf[:count, :], wd[:, cols], preferred_element_type=F32)
            xbuf[:, a:b, cols] = out.astype(BF16).reshape(8, span, tile)
            return _

        lax.fori_loop(0, width // tile, down_tile, 0)
        rows, cols = pl.ds(a, span), pl.ds(0, width)
        rs[c][0] = remote(
            xbuf.at[pl.ds(4, 4), rows, cols], pr.at[:, rows], rss.at[c, 0], rsv.at[c, 0], partner
        )
        rs[c][0].start()

    def add(dst, dst_at, srcs, a, b, low, high):
        tile = 512

        def step(n, _):
            cols = pl.ds(pl.multiple_of(low + n * tile, tile), tile)
            total = dst[dst_at, a:b, cols].astype(F32)
            for src in srcs:
                total = total + src(n * tile, tile).astype(F32)
            dst[dst_at, a:b, cols] = total.astype(BF16)
            return _

        lax.fori_loop(0, (high - low) // tile, step, 0)

    def cut(ref, lead, a, b, base):
        def get(at, size):
            cols = pl.ds(pl.multiple_of(base + at, size), size)
            return ref[a:b, cols] if lead is None else ref[lead, a:b, cols]

        return get

    def partner_sum(c):
        a, b = chunks[c]
        rows = pl.ds(a, b - a)
        low, high = pl.ds(0, half), pl.ds(half, half)
        rs[c][0].wait_recv()
        rs[c][1] = remote(xbuf.at[2, rows, low], ra.at[rows], rss.at[c, 1], rsv.at[c, 1], right)
        rs[c][2] = remote(xbuf.at[2, rows, high], rb.at[rows], rss.at[c, 2], rsv.at[c, 2], left)
        rs[c][3] = remote(
            xbuf.at[1, rows, high], fl.at[rows, high], rss.at[c, 3], rsv.at[c, 3], right
        )
        rs[c][4] = remote(
            xbuf.at[3, rows, low], fr.at[rows, low], rss.at[c, 4], rsv.at[c, 4], left
        )
        rs[c][5] = remote(
            xbuf.at[1, rows, low], fl.at[rows, low], rss.at[c, 5], rsv.at[c, 5], right
        )
        rs[c][6] = remote(
            xbuf.at[3, rows, high], fr.at[rows, high], rss.at[c, 6], rsv.at[c, 6], left
        )
        add(xbuf, 2, [cut(pr, 2, a, b, 0)], a, b, 0, width)
        rs[c][1].start()
        rs[c][2].start()
        add(xbuf, 1, [cut(pr, 1, a, b, 0)], a, b, 0, width)
        rs[c][3].start()
        add(xbuf, 3, [cut(pr, 3, a, b, 0)], a, b, 0, width)
        rs[c][4].start()
        add(xbuf, 0, [cut(pr, 0, a, b, 0)], a, b, 0, width)

    def ring_sum(c):
        a, b = chunks[c]
        rs[c][1].wait_recv()
        add(xbuf, 1, [cut(ra, None, a, b, 0)], a, b, 0, half)
        rs[c][5].start()
        rs[c][2].wait_recv()
        add(xbuf, 3, [cut(rb, None, a, b, 0)], a, b, half, width)
        rs[c][6].start()

    def finish(c):
        a, b = chunks[c]
        for q in (3, 4, 5, 6):
            rs[c][q].wait_recv()
        add(xbuf, 0, [cut(fl, None, a, b, 0), cut(fr, None, a, b, 0)], a, b, 0, width)
        p0 = state["returned"]
        p1 = b // CAP
        state["returned"] = p1
        w0 = p0 * CAP // 16 * 16

        def hit(i, j):
            match = None
            for p in range(p0, p1):
                s = i - (p - p0) * SLOTS
                m = (s >= 0) & (s < CAP) & (j + w0 == s + p * CAP)
                match = m if match is None else match | m
            return match

        spread = onehot((p1 - p0) * SLOTS, b - w0, hit)
        tile = 1280

        def step(n, _):
            cols = pl.ds(pl.multiple_of(n * tile, tile), tile)
            out = jnp.dot(spread, xbuf[0, w0:b, cols], preferred_element_type=F32)
            exr[p0 * SLOTS : p1 * SLOTS, cols] = out.astype(BF16)
            return _

        lax.fori_loop(0, width // tile, step, 0)
        for p in range(p0, p1):
            src = exr.at[pl.ds(p * SLOTS, SLOTS), pl.ds(0, width)]
            if p == 0:
                ret[p] = pltpu.make_async_copy(src, back_ref.at[0], rts.at[0])
            else:
                ret[p] = remote(src, back_ref.at[p], rts.at[p], rtv.at[p], back_there(p))
            ret[p].start()

    last = len(chunks) - 1
    own(0)
    own(1)
    relay(0)
    own(2)
    for w in weights:
        w.wait()
    for c in range(len(chunks)):
        far(c)
        compute(c)
        if c + 1 <= last:
            relay(c + 1)
        if c + 3 <= last:
            own(c + 3)
        partner_sum(c)
        if c >= 1:
            ring_sum(c - 1)
        if c >= 2:
            finish(c - 2)
    ring_sum(last)
    finish(last - 1)
    finish(last)
    for p in range(1, nodes):
        exchange[p].wait_send()
    for c in range(len(chunks)):
        for q in range(7):
            rs[c][q].wait_send()
    ret[0].wait()
    for p in range(1, nodes):
        ret[p].wait_send()
        ret[p].wait_recv()


def routed(send, gate_proj, up_proj, down_proj):
    nodes, slots, ext = send.shape
    local, hidden, width = gate_proj.shape
    rows = nodes * CAP
    chunks = len(CUTS) - 1
    most = max(b - a for a, b in zip(CUTS[:-1], CUTS[1:]))
    tiles = -(-local * hidden // LANES)
    dma = pltpu.SemaphoreType.DMA
    return pl.pallas_call(
        kernel,
        out_shape=jax.ShapeDtypeStruct((nodes, slots, width), BF16),
        in_specs=[pl.BlockSpec(memory_space=pl.ANY)] * 4,
        out_specs=pl.BlockSpec(memory_space=pl.ANY),
        scratch_shapes=[
            pltpu.VMEM((tiles, 2 * LANES, width), BF16),
            pltpu.VMEM((tiles * LANES, width), BF16),
            pltpu.VMEM((8, rows, ext), BF16),
            pltpu.VMEM((nodes * slots, ext), BF16),
            pltpu.VMEM((4, rows, width), BF16),
            pltpu.VMEM((rows, width // 2), BF16),
            pltpu.VMEM((rows, width // 2), BF16),
            pltpu.VMEM((rows, width), BF16),
            pltpu.VMEM((rows, width), BF16),
            pltpu.VMEM((8 * most, tiles * LANES), BF16),
            dma((local * (2 * (hidden // BLOCK) + 1),)),
            dma((nodes,)),
            dma((nodes,)),
            dma((chunks, 8)),
            dma((chunks, 8)),
            dma((chunks, 7)),
            dma((chunks, 7)),
            dma((nodes,)),
            dma((nodes,)),
        ],
        compiler_params=pltpu.CompilerParams(
            collective_id=0, has_side_effects=True, vmem_limit_bytes=67_043_328
        ),
        name="routed_experts",
    )(send, gate_proj, up_proj, down_proj)


def shards(tokens, node_ids, expert_pick, gate_share, gate_proj, up_proj, down_proj):
    tok_count, width = tokens.shape
    nodes = lax.axis_size("node")
    side = math.isqrt(nodes)
    me = lax.axis_index("node")
    choices = node_ids.shape[1]
    local = gate_proj.shape[0]

    hop = jnp.array(HOPS, jnp.int32)
    order = (me // side + hop[:, 0]) % side * side + (me % side + hop[:, 1]) % side
    picked = (
        expert_pick[:, :, None] == jnp.arange(choices * local, dtype=jnp.int32)[None, None, :]
    )
    shares = jnp.sum(jnp.where(picked, gate_share[:, :, None].astype(F32), 0.0), axis=1)
    shares = shares.reshape(tok_count, choices, local)
    chosen = node_ids[:, :, None] == order[None, None, :]
    gates = jnp.sum(
        jnp.where(chosen[:, :, :, None], shares[:, :, None, :], 0.0), axis=1
    )
    mask = jnp.any(chosen, axis=1)
    at = jnp.arange(tok_count, dtype=jnp.int32)
    earlier = (at[None, :] < at[:, None]).astype(BF16)
    before = jnp.dot(earlier, mask.astype(BF16), preferred_element_type=F32).astype(jnp.int32)
    slot_of = jnp.where(mask, before, -1)
    select = (
        slot_of.T[:, None, :] == jnp.arange(SLOTS, dtype=jnp.int32)[None, :, None]
    ).astype(BF16)
    flat = select.reshape(nodes * SLOTS, tok_count)
    feats = jnp.dot(flat, tokens, preferred_element_type=F32).astype(BF16)
    gate_rows = jnp.einsum(
        "pst,tpe->pse", select, gates.astype(BF16), preferred_element_type=F32
    ).astype(BF16)
    gate_rows = jnp.pad(gate_rows, ((0, 0), (0, 0), (0, LANES - local)))
    send = jnp.concatenate([feats.reshape(nodes, SLOTS, width), gate_rows], axis=2)

    back = routed(send, gate_proj, up_proj, down_proj)
    total = lax.dot_general(
        flat, back.reshape(nodes * SLOTS, width), (((0,), (0,)), ((), ())),
        preferred_element_type=F32,
    )
    return total.astype(BF16)


def solution(mesh):
    return jax.shard_map(
        shards,
        mesh=mesh,
        in_specs=(
            P(("node", "dev"), None),
            P(("node", "dev"), None),
            P(("node", "dev"), None),
            P(("node", "dev"), None),
            P("node", "dev", None),
            P("node", "dev", None),
            P("node", "dev", None),
        ),
        out_specs=P(("node", "dev"), None),
        check_vma=False,
    )
```

```python
import math

import jax
import jax.numpy as jnp
from jax import lax
from jax.experimental import pallas as pl
from jax.experimental.pallas import tpu as pltpu
from jax.sharding import PartitionSpec as P

LANES = 128
SLOTS = 16
CAP = 13
BLOCK = 64
WB = 512
F32 = jnp.float32
BF16 = jnp.bfloat16
MESH = pl.DeviceIdType.MESH
CUTS = (0, 48, 112, 176, 208)
HOPS = (
    (0, 0), (0, 1), (1, 0), (0, 3), (1, 1), (3, 3), (0, 2), (2, 0),
    (1, 2), (2, 3), (2, 1), (3, 2), (2, 2), (3, 1), (1, 3), (3, 0),
)


def kernel(
    ids_ref, pick_ref, share_ref, tok_ref, gate_ref, up_ref, down_ref, out_ref,
    tbuf, sbuf, tb, pb, selb, xs, er, back, wgu, wd, xbuf, exr, pr, ra, rb, fl, fr, hbuf,
    tsem, tss, trs, bxs, bxr, wsem, exs, exv, ags, agv, rss, rsv, rts, rtv,
):
    local, hidden, width = gate_ref.shape
    nodes = len(HOPS)
    side = math.isqrt(nodes)
    half = width // 2
    da = width - 2 * WB
    ext = da + LANES
    tiles = wgu.shape[0]
    node = lax.axis_index("node")
    dev = lax.axis_index("dev")
    z, y = node // side, node % side
    ring = 4
    cx, core = dev // 2, dev % 2
    right = {"dev": (cx + 1) % ring * 2 + core}
    left = {"dev": (cx + ring - 1) % ring * 2 + core}
    partner = {"dev": cx * 2 + (1 - core)}

    def there(p):
        dz, dy = HOPS[p]
        return {"node": (z + dz) % side * side + (y + dy) % side}

    def back_there(p):
        dz, dy = HOPS[p]
        return {"node": (z + side - dz) % side * side + (y + side - dy) % side}

    def remote(src, dst, ssem, rsem, device):
        return pltpu.make_async_remote_copy(
            src_ref=src, dst_ref=dst, send_sem=ssem, recv_sem=rsem,
            device_id=device, device_id_type=MESH,
        )

    mine_at = pl.multiple_of(da + core * WB, LANES)
    other_at = pl.multiple_of(da + (1 - core) * WB, LANES)
    pieces = (
        (pl.ds(0, da), pl.ds(0, da)),
        (pl.ds(mine_at, WB), pl.ds(da, WB)),
        (pl.ds(other_at, WB), pl.ds(da + WB, WB)),
    )

    weights = []
    for e in range(local):
        for b in range(hidden // BLOCK):
            blk = e * (hidden // BLOCK) + b
            i, at = blk // 2, blk % 2 * BLOCK
            rows = pl.ds(b * BLOCK, BLOCK)
            for src, dst in pieces:
                weights.append(
                    (gate_ref.at[e, rows, src], wgu.at[i, pl.ds(at, BLOCK), dst])
                )
                weights.append(
                    (up_ref.at[e, rows, src], wgu.at[i, pl.ds(LANES + at, BLOCK), dst])
                )
        weights.append((down_ref.at[e], wd.at[pl.ds(e * hidden, hidden)]))
    weights = [
        pltpu.make_async_copy(s, d, wsem.at[i]) for i, (s, d) in enumerate(weights)
    ]

    barrier = pltpu.get_barrier_semaphore()
    for p in range(1, nodes):
        pl.semaphore_signal(barrier, inc=1, device_id=there(p), device_id_type=MESH)
    for device in (right, left, partner):
        pl.semaphore_signal(barrier, inc=1, device_id=device, device_id_type=MESH)
    token_copies = [
        pltpu.make_async_copy(tok_ref.at[:, src], tbuf.at[:, dst], tsem.at[i])
        for i, (src, dst) in enumerate(pieces)
    ]
    for copy in token_copies:
        copy.start()
    for w in weights:
        w.start()
    used = local * hidden
    if used < tiles * LANES:
        rest = tiles * LANES - used
        wgu[tiles - 1, LANES - rest : LANES] = jnp.zeros((rest, width), BF16)
        wgu[tiles - 1, 2 * LANES - rest :] = jnp.zeros((rest, width), BF16)
        wd[used:] = jnp.zeros((rest, width), BF16)
    def onehot(rows, cols, hit):
        i = lax.broadcasted_iota(jnp.int32, (rows, cols), 0)
        j = lax.broadcasted_iota(jnp.int32, (rows, cols), 1)
        return hit(i, j).astype(F32).astype(BF16)

    count_tok, choices = ids_ref.shape
    wide = (count_tok, nodes * SLOTS)
    lane = lax.broadcasted_iota(jnp.int32, wide, 1)
    group, slot = lane // SLOTS, lane % SLOTS
    order = jnp.zeros(wide, jnp.int32)
    for p in range(nodes):
        order = jnp.where(group == p, there(p)["node"], order)
    hits = [ids_ref[:, m : m + 1] == order for m in range(choices)]
    mask = hits[0]
    for m in range(1, choices):
        mask = mask | hits[m]
    earlier = onehot(count_tok, count_tok, lambda i, j: j < i)
    rank = jnp.dot(earlier, mask.astype(F32).astype(BF16), preferred_element_type=F32)
    select = jnp.where(mask & (rank == slot.astype(F32)), 1.0, 0.0)
    rows_of = select.T.astype(BF16)
    gate_rows = jnp.zeros((nodes * SLOTS, LANES), F32)
    for e in range(local):
        gates = jnp.zeros(wide, F32)
        for m in range(choices):
            share = jnp.zeros((count_tok, 1), F32)
            for k in range(pick_ref.shape[1]):
                share = share + jnp.where(
                    pick_ref[:, k : k + 1] == m * local + e,
                    share_ref[:, k : k + 1].astype(F32),
                    0.0,
                )
            gates = gates + jnp.where(hits[m], share, 0.0)
        gate_rows = gate_rows + jnp.dot(
            (select * gates).T.astype(BF16),
            onehot(count_tok, LANES, lambda i, j: j == e),
            preferred_element_type=F32,
        )
    sbuf[:, da:] = gate_rows.astype(BF16)
    spread_rows = select.astype(BF16)
    slots_of = jnp.dot(
        jnp.where(mask, rank, -1.0).astype(BF16),
        onehot(nodes * SLOTS, LANES, lambda i, j: i == j * SLOTS),
        preferred_element_type=F32,
    )
    slots_of = jnp.where(
        lax.broadcasted_iota(jnp.int32, slots_of.shape, 1) < nodes, slots_of, -1.0
    ).astype(BF16)
    for copy in token_copies:
        copy.wait()
    tb[0, :count_tok, :WB] = tbuf[:, da : da + WB]
    tb[0, :count_tok, WB:] = slots_of
    pb[:, :WB] = tbuf[:, da + WB :]
    pb[:, WB:] = slots_of

    def pack(n, _):
        cols = pl.ds(pl.multiple_of(n * 1024, 1024), 1024)
        sbuf[:, cols] = jnp.dot(
            rows_of, tbuf[:, cols], preferred_element_type=F32
        ).astype(BF16)
        return _

    lax.fori_loop(0, da // 1024, pack, 0)
    exr[:SLOTS, :ext] = sbuf[:SLOTS, :]
    pl.semaphore_wait(barrier, nodes + 2)

    first, second = pl.ds(0, count_tok), pl.ds(count_tok, count_tok)
    row = [
        remote(pb, tb.at[0, second], tss.at[0], trs.at[0], partner),
        remote(tb.at[0, first], tb.at[3, first], tss.at[1], trs.at[1], right),
        remote(tb.at[0, second], tb.at[3, second], tss.at[2], trs.at[2], right),
        remote(tb.at[0, second], tb.at[1, second], tss.at[3], trs.at[3], left),
        remote(tb.at[0, first], tb.at[1, first], tss.at[4], trs.at[4], left),
        remote(tb.at[3, first], tb.at[2, first], tss.at[5], trs.at[5], right),
        remote(tb.at[1, second], tb.at[2, second], tss.at[6], trs.at[6], left),
    ]
    for q in (0, 1, 4):
        row[q].start()
    exchange = {}

    def exchange_rows(c):
        p0, p1 = starts[c], starts[c + 1]
        for p in range(max(p0, 1), p1):
            block = pl.ds(p * SLOTS, SLOTS)
            exchange[p] = remote(
                sbuf.at[block], exr.at[block, pl.ds(0, ext)], exs.at[p], exv.at[p], there(p)
            )
            exchange[p].start()

    chunks = list(zip(CUTS[:-1], CUTS[1:]))
    starts = [0] + [(b - 1) // CAP + 1 for _, b in chunks]
    ag = [{} for _ in chunks]
    rs = [{} for _ in chunks]
    state = {"arrived": 0, "returned": 0}
    ret = {}

    low, high = pl.ds(0, half), pl.ds(half, half)
    ag_low, ag_high, ag_all = pl.ds(0, da // 2), pl.ds(da // 2, ext - da // 2), pl.ds(0, ext)
    bsend = {}

    def selectors(dx):
        for dc in range(2):
            vals = tb[dx, dc * count_tok : (dc + 1) * count_tok, WB:]
            wanted = jnp.dot(
                vals,
                onehot(LANES, nodes * SLOTS, lambda i, j: i == j // SLOTS),
                preferred_element_type=F32,
            )
            hit = jnp.where(wanted == slot.astype(F32), 1.0, 0.0)
            selb[dx * 2 + dc] = hit.T.astype(BF16)

    def build(c):
        p0, p1 = starts[c], starts[c + 1]
        if c >= 2:
            for p in range(max(starts[c - 2], 1), starts[c - 1]):
                bsend[p].wait_send()
        for k in range(8):
            tok = tb[k // 2, k % 2 * count_tok : (k % 2 + 1) * count_tok, :WB]
            rows = jnp.dot(
                selb[k, p0 * SLOTS : p1 * SLOTS, :], tok, preferred_element_type=F32
            ).astype(BF16)
            rows = rows.reshape(p1 - p0, SLOTS, WB)
            if p0 == 0:
                er[0, k] = rows[0]
            xs[c % 2, : p1 - p0, k] = rows
        for p in range(max(p0, 1), p1):
            bsend[p] = remote(
                xs.at[c % 2, p - p0], er.at[p], bxs.at[p], bxr.at[p], there(p)
            )
            bsend[p].start()

    def picker(c):
        a, b = chunks[c]
        n0, n1 = a // CAP, (b - 1) // CAP + 1

        def hit(i, j):
            match = None
            for p in range(n0, n1):
                k = j - (p - n0) * SLOTS
                m = (k >= 0) & (k < CAP) & (i + a == k + p * CAP)
                match = m if match is None else match | m
            return match

        return onehot(b - a, (n1 - n0) * SLOTS, hit), n0, n1

    def take(c):
        a, b = chunks[c]
        for p in range(max(starts[c], 1), starts[c + 1]):
            bsend[p].wait_recv()
        pick, n0, n1 = picker(c)
        for k in range(8):
            src = er[n0:n1, k].reshape((n1 - n0) * SLOTS, WB)
            xbuf[k % 2 * 4 + k // 2, a:b, ext : ext + WB] = jnp.dot(
                pick, src, preferred_element_type=F32
            ).astype(BF16)
        rows = pl.ds(a, b - a)
        for q, s in ((10, 0), (11, 4)):
            ag[c][q] = remote(
                xbuf.at[pl.ds(s, 4), rows, pl.ds(ext, WB)],
                xbuf.at[pl.ds(4 - s, 4), rows, pl.ds(ext + WB, WB)],
                ags.at[c, q], agv.at[c, q], partner,
            )
            ag[c][q].start()

    def own(c):
        a, b = chunks[c]
        for p in range(max(starts[c], 1), starts[c + 1]):
            exchange[p].wait_recv()
        pick, n0, n1 = picker(c)
        dense = jnp.dot(
            pick, exr[n0 * SLOTS : n1 * SLOTS, :ext], preferred_element_type=F32
        )
        xbuf[0, a:b, :ext] = dense.astype(BF16)
        rows = pl.ds(a, b - a)
        for q, s, cols, device in (
            (0, 3, ag_low, right), (2, 1, ag_high, left),
            (1, 3, ag_high, right), (3, 1, ag_low, left),
        ):
            ag[c][q] = remote(
                xbuf.at[0, rows, cols], xbuf.at[s, rows, cols], ags.at[c, q], agv.at[c, q], device
            )
            ag[c][q].start()
        ag[c][4] = remote(
            xbuf.at[0, rows, ag_all], xbuf.at[4, rows, ag_all], ags.at[c, 4], agv.at[c, 4], partner
        )
        ag[c][4].start()

    def relay(c):
        a, b = chunks[c]
        rows = pl.ds(a, b - a)
        ag[c][5] = remote(
            xbuf.at[3, rows, ag_low], xbuf.at[2, rows, ag_low], ags.at[c, 5], agv.at[c, 5], right
        )
        ag[c][6] = remote(
            xbuf.at[1, rows, ag_high], xbuf.at[2, rows, ag_high], ags.at[c, 6], agv.at[c, 6], left
        )
        ag[c][0].wait_recv()
        ag[c][5].start()
        ag[c][2].wait_recv()
        ag[c][6].start()

    def forward(c):
        a, b = chunks[c]
        rows = pl.ds(a, b - a)
        for q, s, ready in ((7, 3, 1), (8, 1, 3)):
            ag[c][ready].wait_recv()
            ag[c][q] = remote(
                xbuf.at[s, rows, ag_all], xbuf.at[4 + s, rows, ag_all],
                ags.at[c, q], agv.at[c, q], partner,
            )
            ag[c][q].start()

    def far(c):
        a, b = chunks[c]
        rows = pl.ds(a, b - a)
        ag[c][5].wait_recv()
        ag[c][6].wait_recv()
        ag[c][9] = remote(
            xbuf.at[2, rows, ag_all], xbuf.at[6, rows, ag_all], ags.at[c, 9], agv.at[c, 9], partner
        )
        ag[c][9].start()
        for q in (4, 7, 8, 9, 10, 11):
            ag[c][q].wait_recv()

    def gated(c, first, count_tiles):
        a, b = chunks[c]
        span = b - a
        count = 8 * span

        def hidden_tile(i, _):
            contract = (((1,), (1,)), ((), ()))
            acc = lax.dot_general(
                xbuf[:, a:b, :da].reshape(count, da), wgu[i, :, :da], contract,
                preferred_element_type=F32,
            ) + lax.dot_general(
                xbuf[:, a:b, ext:].reshape(count, 2 * WB), wgu[i, :, da:], contract,
                preferred_element_type=F32,
            )
            g, u = acc[:, :LANES], acc[:, LANES:]
            shares = xbuf[:, a:b, da:ext].reshape(count, LANES)

            def hit(e, j):
                at = j + i * LANES - e * hidden
                return (at >= 0) & (at < hidden) & (e < local)

            scale = jnp.dot(
                shares, onehot(LANES, LANES, hit), preferred_element_type=F32
            )
            h = g / (1.0 + jnp.exp(-g)) * u * scale
            hbuf[:count, pl.ds(pl.multiple_of(i * LANES, LANES), LANES)] = h.astype(BF16)
            return _

        lax.fori_loop(first, first + count_tiles, hidden_tile, 0)

    def sent(c):
        for q in range(12):
            ag[c][q].wait_send()

    def down(c, q):
        a, b = chunks[c]
        span = b - a
        count = 8 * span
        tile = 512

        def down_tile(n, _):
            cols = pl.ds(pl.multiple_of(q * half + n * tile, tile), tile)
            out = jnp.dot(hbuf[:count, :], wd[:, cols], preferred_element_type=F32)
            xbuf[:, a:b, cols] = out.astype(BF16).reshape(8, span, tile)
            return _

        lax.fori_loop(0, half // tile, down_tile, 0)
        rows, cols = pl.ds(a, span), (low, high)[q]
        rs[c][q] = remote(
            xbuf.at[pl.ds(4, 4), rows, cols], pr.at[c % 2, :, pl.ds(0, span), cols],
            rss.at[c, q], rsv.at[c, q], partner,
        )
        rs[c][q].start()

    def add(dst, dst_at, srcs, a, b, low, high):
        tile = 512

        def step(n, _):
            cols = pl.ds(pl.multiple_of(low + n * tile, tile), tile)
            total = dst[dst_at, a:b, cols].astype(F32)
            for src in srcs:
                total = total + src(n * tile, tile).astype(F32)
            dst[dst_at, a:b, cols] = total.astype(BF16)
            return _

        lax.fori_loop(0, (high - low) // tile, step, 0)

    def cut(ref, lead, a, b, base):
        def get(at, size):
            cols = pl.ds(pl.multiple_of(base + at, size), size)
            return ref[a:b, cols] if lead is None else ref[lead, a:b, cols]

        return get

    def partner_sum(c, q):
        a, b = chunks[c]
        rows, cols = pl.ds(a, b - a), (low, high)[q]
        at, to = q * half, (q + 1) * half
        rs[c][q].wait_recv()
        far_to, landing = (right, ra) if q == 0 else (left, rb)
        near, near_to, near_at = (3, left, fr) if q == 0 else (1, right, fl)
        add(xbuf, 2, [cut(pr.at[c % 2, 2], None, 0, b - a, at)], a, b, at, to)
        rs[c][2 + q] = remote(
            xbuf.at[2, rows, cols], landing.at[rows], rss.at[c, 2 + q], rsv.at[c, 2 + q], far_to
        )
        rs[c][2 + q].start()
        add(xbuf, near, [cut(pr.at[c % 2, near], None, 0, b - a, at)], a, b, at, to)
        rs[c][4 + q] = remote(
            xbuf.at[near, rows, cols], near_at.at[rows, cols],
            rss.at[c, 4 + q], rsv.at[c, 4 + q], near_to,
        )
        rs[c][4 + q].start()
        add(xbuf, 4 - near, [cut(pr.at[c % 2, 4 - near], None, 0, b - a, at)], a, b, at, to)
        add(xbuf, 0, [cut(pr.at[c % 2, 0], None, 0, b - a, at)], a, b, at, to)

    def ring_sum(c):
        a, b = chunks[c]
        rows = pl.ds(a, b - a)
        for q, s, landed, to, at in ((0, 1, ra, right, fl), (1, 3, rb, left, fr)):
            cols = (low, high)[q]
            rs[c][2 + q].wait_recv()
            add(xbuf, s, [cut(landed, None, a, b, 0)], a, b, q * half, (q + 1) * half)
            rs[c][6 + q] = remote(
                xbuf.at[s, rows, cols], at.at[rows, cols], rss.at[c, 6 + q], rsv.at[c, 6 + q], to
            )
            rs[c][6 + q].start()

    def finish(c):
        a, b = chunks[c]
        for q in (4, 5, 6, 7):
            rs[c][q].wait_recv()
        add(xbuf, 0, [cut(fl, None, a, b, 0), cut(fr, None, a, b, 0)], a, b, 0, width)
        p0 = state["returned"]
        p1 = b // CAP
        state["returned"] = p1
        w0 = p0 * CAP // 16 * 16

        def hit(i, j):
            match = None
            for p in range(p0, p1):
                s = i - (p - p0) * SLOTS
                m = (s >= 0) & (s < CAP) & (j + w0 == s + p * CAP)
                match = m if match is None else match | m
            return match

        spread = onehot((p1 - p0) * SLOTS, b - w0, hit)
        tile = 1280

        def step(n, _):
            cols = pl.ds(pl.multiple_of(n * tile, tile), tile)
            out = jnp.dot(spread, xbuf[0, w0:b, cols], preferred_element_type=F32)
            exr[p0 * SLOTS : p1 * SLOTS, cols] = out.astype(BF16)
            return _

        lax.fori_loop(0, width // tile, step, 0)
        for p in range(p0, p1):
            block = pl.ds(p * SLOTS, SLOTS)
            if p == 0:
                back[:SLOTS, :] = exr[:SLOTS, :width]
            else:
                ret[p] = remote(
                    exr.at[block, pl.ds(0, width)], back.at[block], rts.at[p], rtv.at[p], back_there(p)
                )
                ret[p].start()

    last = len(chunks) - 1
    exchange_rows(0)
    row[0].wait_recv()
    row[2].start()
    row[3].start()
    exchange_rows(1)
    selectors(0)
    row[1].wait_recv()
    row[5].start()
    row[3].wait_recv()
    row[6].start()
    own(0)
    row[2].wait_recv()
    selectors(3)
    row[4].wait_recv()
    selectors(1)
    row[5].wait_recv()
    row[6].wait_recv()
    selectors(2)
    build(0)
    exchange_rows(2)
    build(1)
    relay(0)
    own(1)
    for c in range(3, len(chunks)):
        exchange_rows(c)
    forward(0)
    take(0)
    for w in weights:
        w.wait()
    for c in range(len(chunks)):
        far(c)
        gated(c, 0, 2)
        if c + 1 <= last:
            relay(c + 1)
        if c + 2 <= last:
            own(c + 2)
            build(c + 2)
        gated(c, 2, tiles - 2)
        if c + 1 <= last:
            forward(c + 1)
        if c >= 2:
            finish(c - 2)
        if c >= 1:
            ring_sum(c - 1)
        sent(c)
        down(c, 0)
        down(c, 1)
        partner_sum(c, 0)
        partner_sum(c, 1)
        if c + 1 <= last:
            take(c + 1)
    finish(last - 1)
    ring_sum(last)
    finish(last)
    for q in row:
        q.wait_send()
    for p in range(max(starts[-3], 1), nodes):
        bsend[p].wait_send()
    for p in range(1, nodes):
        exchange[p].wait_send()
    for c in range(len(chunks)):
        for q in range(8):
            rs[c][q].wait_send()
    for p in range(1, nodes):
        ret[p].wait_send()
        ret[p].wait_recv()

    def unpack(n, _):
        cols = pl.ds(pl.multiple_of(n * 1280, 1280), 1280)
        out_ref[:, cols] = jnp.dot(
            spread_rows, back[:, cols], preferred_element_type=F32
        ).astype(BF16)
        return _

    lax.fori_loop(0, width // 1280, unpack, 0)


def shards(tokens, node_ids, expert_pick, gate_share, gate_proj, up_proj, down_proj):
    tok_count, width = tokens.shape
    local, hidden, _ = gate_proj.shape
    nodes = len(HOPS)
    rows = nodes * CAP
    chunks = len(CUTS) - 1
    most = max(b - a for a, b in zip(CUTS[:-1], CUTS[1:]))
    starts = [0] + [(b - 1) // CAP + 1 for b in CUTS[1:]]
    groups = max(b - a for a, b in zip(starts[:-1], starts[1:]))
    tiles = -(-local * hidden // LANES)
    dma = pltpu.SemaphoreType.DMA
    vmem, anywhere = pl.BlockSpec(memory_space=pltpu.VMEM), pl.BlockSpec(memory_space=pl.ANY)
    return pl.pallas_call(
        kernel,
        out_shape=jax.ShapeDtypeStruct((tok_count, width), BF16),
        in_specs=[vmem] * 3 + [anywhere] * 4,
        out_specs=vmem,
        scratch_shapes=[
            pltpu.VMEM((tok_count, width), BF16),
            pltpu.VMEM((nodes * SLOTS, width - 2 * WB + LANES), BF16),
            pltpu.VMEM((4, 2 * tok_count, WB + LANES), BF16),
            pltpu.VMEM((tok_count, WB + LANES), BF16),
            pltpu.VMEM((8, nodes * SLOTS, tok_count), BF16),
            pltpu.VMEM((2, groups, 8, SLOTS, WB), BF16),
            pltpu.VMEM((nodes, 8, SLOTS, WB), BF16),
            pltpu.VMEM((nodes * SLOTS, width), BF16),
            pltpu.VMEM((tiles, 2 * LANES, width), BF16),
            pltpu.VMEM((tiles * LANES, width), BF16),
            pltpu.VMEM((8, rows, width + LANES), BF16),
            pltpu.VMEM((nodes * SLOTS, width), BF16),
            pltpu.VMEM((2, 4, most, width), BF16),
            pltpu.VMEM((rows, width // 2), BF16),
            pltpu.VMEM((rows, width // 2), BF16),
            pltpu.VMEM((rows, width), BF16),
            pltpu.VMEM((rows, width), BF16),
            pltpu.VMEM((8 * most, tiles * LANES), BF16),
            dma((3,)),
            dma((7,)),
            dma((7,)),
            dma((nodes,)),
            dma((nodes,)),
            dma((local * (6 * (hidden // BLOCK) + 1),)),
            dma((nodes,)),
            dma((nodes,)),
            dma((chunks, 12)),
            dma((chunks, 12)),
            dma((chunks, 8)),
            dma((chunks, 8)),
            dma((nodes,)),
            dma((nodes,)),
        ],
        compiler_params=pltpu.CompilerParams(
            collective_id=0, has_side_effects=True, vmem_limit_bytes=67_043_328
        ),
        name="routed_experts",
    )(node_ids, expert_pick, gate_share, tokens, gate_proj, up_proj, down_proj)


def solution(mesh):
    return jax.shard_map(
        shards,
        mesh=mesh,
        in_specs=(
            P(("node", "dev"), None),
            P(("node", "dev"), None),
            P(("node", "dev"), None),
            P(("node", "dev"), None),
            P("node", "dev", None),
            P("node", "dev", None),
            P("node", "dev", None),
        ),
        out_specs=P(("node", "dev"), None),
        check_vma=False,
    )
```

```python
import math

import jax
import jax.numpy as jnp
from jax import lax
from jax.experimental import pallas as pl
from jax.experimental.pallas import tpu as pltpu
from jax.sharding import PartitionSpec as P

LANES = 128
SLOTS = 16
CAP = 13
BLOCK = 64
WB = 512
F32 = jnp.float32
BF16 = jnp.bfloat16
MESH = pl.DeviceIdType.MESH
CUTS = (0, 48, 112, 160, 208)
HOPS = (
    (0, 0), (0, 1), (1, 0), (0, 3), (1, 1), (3, 3), (0, 2), (2, 0),
    (1, 2), (2, 3), (2, 1), (3, 2), (2, 2), (3, 1), (1, 3), (3, 0),
)


def kernel(
    ids_ref, pick_ref, share_ref, tok_ref, gate_ref, up_ref, down_ref, out_ref,
    tbuf, sbuf, tb, pb, selb, xs, er, back, wgu, wd, xbuf, exr, pr, ra, rb, fl, fr, hbuf,
    tsem, tss, trs, bxs, bxr, wsem, exs, exv, ags, agv, rss, rsv, rts, rtv,
):
    local, hidden, width = gate_ref.shape
    nodes = len(HOPS)
    side = math.isqrt(nodes)
    half = width // 2
    da = width - 2 * WB
    ext = da + LANES
    tiles = wgu.shape[0]
    node = lax.axis_index("node")
    dev = lax.axis_index("dev")
    z, y = node // side, node % side
    ring = 4
    cx, core = dev // 2, dev % 2
    right = {"dev": (cx + 1) % ring * 2 + core}
    left = {"dev": (cx + ring - 1) % ring * 2 + core}
    partner = {"dev": cx * 2 + (1 - core)}

    def there(p):
        dz, dy = HOPS[p]
        return {"node": (z + dz) % side * side + (y + dy) % side}

    def back_there(p):
        dz, dy = HOPS[p]
        return {"node": (z + side - dz) % side * side + (y + side - dy) % side}

    def remote(src, dst, ssem, rsem, device):
        return pltpu.make_async_remote_copy(
            src_ref=src, dst_ref=dst, send_sem=ssem, recv_sem=rsem,
            device_id=device, device_id_type=MESH,
        )

    mine_at = pl.multiple_of(da + core * WB, LANES)
    other_at = pl.multiple_of(da + (1 - core) * WB, LANES)
    pieces = (
        (pl.ds(0, da), pl.ds(0, da)),
        (pl.ds(mine_at, WB), pl.ds(da, WB)),
        (pl.ds(other_at, WB), pl.ds(da + WB, WB)),
    )

    weights = []
    for e in range(local):
        for b in range(hidden // BLOCK):
            blk = e * (hidden // BLOCK) + b
            i, at = blk // 2, blk % 2 * BLOCK
            rows = pl.ds(b * BLOCK, BLOCK)
            for src, dst in pieces:
                weights.append(
                    (gate_ref.at[e, rows, src], wgu.at[i, pl.ds(at, BLOCK), dst])
                )
                weights.append(
                    (up_ref.at[e, rows, src], wgu.at[i, pl.ds(LANES + at, BLOCK), dst])
                )
        weights.append((down_ref.at[e], wd.at[pl.ds(e * hidden, hidden)]))
    weights = [
        pltpu.make_async_copy(s, d, wsem.at[i]) for i, (s, d) in enumerate(weights)
    ]

    barrier = pltpu.get_barrier_semaphore()
    for p in range(1, nodes):
        pl.semaphore_signal(barrier, inc=1, device_id=there(p), device_id_type=MESH)
    for device in (right, left, partner):
        pl.semaphore_signal(barrier, inc=1, device_id=device, device_id_type=MESH)
    token_copies = [
        pltpu.make_async_copy(tok_ref.at[:, src], tbuf.at[:, dst], tsem.at[i])
        for i, (src, dst) in enumerate(pieces)
    ]
    for copy in token_copies:
        copy.start()
    for w in weights:
        w.start()
    used = local * hidden
    if used < tiles * LANES:
        rest = tiles * LANES - used
        wgu[tiles - 1, LANES - rest : LANES] = jnp.zeros((rest, width), BF16)
        wgu[tiles - 1, 2 * LANES - rest :] = jnp.zeros((rest, width), BF16)
        wd[used:] = jnp.zeros((rest, width), BF16)
    def onehot(rows, cols, hit):
        i = lax.broadcasted_iota(jnp.int32, (rows, cols), 0)
        j = lax.broadcasted_iota(jnp.int32, (rows, cols), 1)
        return hit(i, j).astype(F32).astype(BF16)

    count_tok, choices = ids_ref.shape
    wide = (count_tok, nodes * SLOTS)
    lane = lax.broadcasted_iota(jnp.int32, wide, 1)
    group, slot = lane // SLOTS, lane % SLOTS
    order = jnp.zeros(wide, jnp.int32)
    for p in range(nodes):
        order = jnp.where(group == p, there(p)["node"], order)
    hits = [ids_ref[:, m : m + 1] == order for m in range(choices)]
    mask = hits[0]
    for m in range(1, choices):
        mask = mask | hits[m]
    earlier = onehot(count_tok, count_tok, lambda i, j: j < i)
    rank = jnp.dot(earlier, mask.astype(F32).astype(BF16), preferred_element_type=F32)
    select = jnp.where(mask & (rank == slot.astype(F32)), 1.0, 0.0)
    rows_of = select.T.astype(BF16)
    gate_rows = jnp.zeros((nodes * SLOTS, LANES), F32)
    for e in range(local):
        gates = jnp.zeros(wide, F32)
        for m in range(choices):
            share = jnp.zeros((count_tok, 1), F32)
            for k in range(pick_ref.shape[1]):
                share = share + jnp.where(
                    pick_ref[:, k : k + 1] == m * local + e,
                    share_ref[:, k : k + 1].astype(F32),
                    0.0,
                )
            gates = gates + jnp.where(hits[m], share, 0.0)
        gate_rows = gate_rows + jnp.dot(
            (select * gates).T.astype(BF16),
            onehot(count_tok, LANES, lambda i, j: j == e),
            preferred_element_type=F32,
        )
    sbuf[:, da:] = gate_rows.astype(BF16)
    spread_rows = select.astype(BF16)
    slots_of = jnp.dot(
        jnp.where(mask, rank, -1.0).astype(BF16),
        onehot(nodes * SLOTS, LANES, lambda i, j: i == j * SLOTS),
        preferred_element_type=F32,
    )
    slots_of = jnp.where(
        lax.broadcasted_iota(jnp.int32, slots_of.shape, 1) < nodes, slots_of, -1.0
    ).astype(BF16)
    for copy in token_copies:
        copy.wait()
    tb[0, :count_tok, :WB] = tbuf[:, da : da + WB]
    tb[0, :count_tok, WB:] = slots_of
    pb[:, :WB] = tbuf[:, da + WB :]
    pb[:, WB:] = slots_of

    def pack(n, _):
        cols = pl.ds(pl.multiple_of(n * 1024, 1024), 1024)
        sbuf[:, cols] = jnp.dot(
            rows_of, tbuf[:, cols], preferred_element_type=F32
        ).astype(BF16)
        return _

    lax.fori_loop(0, da // 1024, pack, 0)
    exr[:SLOTS, :ext] = sbuf[:SLOTS, :]
    pl.semaphore_wait(barrier, nodes + 2)

    first, second = pl.ds(0, count_tok), pl.ds(count_tok, count_tok)
    row = [
        remote(pb, tb.at[0, second], tss.at[0], trs.at[0], partner),
        remote(tb.at[0, first], tb.at[3, first], tss.at[1], trs.at[1], right),
        remote(tb.at[0, second], tb.at[3, second], tss.at[2], trs.at[2], right),
        remote(tb.at[0, second], tb.at[1, second], tss.at[3], trs.at[3], left),
        remote(tb.at[0, first], tb.at[1, first], tss.at[4], trs.at[4], left),
        remote(tb.at[3, first], tb.at[2, first], tss.at[5], trs.at[5], right),
        remote(tb.at[1, second], tb.at[2, second], tss.at[6], trs.at[6], left),
    ]
    for q in (0, 1, 4):
        row[q].start()
    exchange = {}

    def exchange_rows(c):
        p0, p1 = starts[c], starts[c + 1]
        for p in range(max(p0, 1), p1):
            block = pl.ds(p * SLOTS, SLOTS)
            exchange[p] = remote(
                sbuf.at[block], exr.at[block, pl.ds(0, ext)], exs.at[p], exv.at[p], there(p)
            )
            exchange[p].start()

    chunks = list(zip(CUTS[:-1], CUTS[1:]))
    starts = [0] + [(b - 1) // CAP + 1 for _, b in chunks]
    ag = [{} for _ in chunks]
    rs = [{} for _ in chunks]
    state = {"arrived": 0, "returned": 0}
    ret = {}

    low, high = pl.ds(0, half), pl.ds(half, half)
    ag_low, ag_high, ag_all = pl.ds(0, da // 2), pl.ds(da // 2, ext - da // 2), pl.ds(0, ext)
    bsend = {}

    def selectors(dx):
        for dc in range(2):
            vals = tb[dx, dc * count_tok : (dc + 1) * count_tok, WB:]
            wanted = jnp.dot(
                vals,
                onehot(LANES, nodes * SLOTS, lambda i, j: i == j // SLOTS),
                preferred_element_type=F32,
            )
            hit = jnp.where(wanted == slot.astype(F32), 1.0, 0.0)
            selb[dx * 2 + dc] = hit.T.astype(BF16)

    def build(c):
        p0, p1 = starts[c], starts[c + 1]
        if c >= 2:
            for p in range(max(starts[c - 2], 1), starts[c - 1]):
                bsend[p].wait_send()
        for k in range(8):
            tok = tb[k // 2, k % 2 * count_tok : (k % 2 + 1) * count_tok, :WB]
            rows = jnp.dot(
                selb[k, p0 * SLOTS : p1 * SLOTS, :], tok, preferred_element_type=F32
            ).astype(BF16)
            rows = rows.reshape(p1 - p0, SLOTS, WB)
            if p0 == 0:
                er[0, k] = rows[0]
            xs[c % 2, : p1 - p0, k] = rows
        for p in range(max(p0, 1), p1):
            bsend[p] = remote(
                xs.at[c % 2, p - p0], er.at[p], bxs.at[p], bxr.at[p], there(p)
            )
            bsend[p].start()

    def picker(c):
        a, b = chunks[c]
        n0, n1 = a // CAP, (b - 1) // CAP + 1

        def hit(i, j):
            match = None
            for p in range(n0, n1):
                k = j - (p - n0) * SLOTS
                m = (k >= 0) & (k < CAP) & (i + a == k + p * CAP)
                match = m if match is None else match | m
            return match

        return onehot(b - a, (n1 - n0) * SLOTS, hit), n0, n1

    def take(c):
        a, b = chunks[c]
        for p in range(max(starts[c], 1), starts[c + 1]):
            bsend[p].wait_recv()
        pick, n0, n1 = picker(c)
        for k in range(8):
            src = er[n0:n1, k].reshape((n1 - n0) * SLOTS, WB)
            xbuf[k % 2 * 4 + k // 2, a:b, ext : ext + WB] = jnp.dot(
                pick, src, preferred_element_type=F32
            ).astype(BF16)
        rows = pl.ds(a, b - a)
        for q, s in ((10, 0), (11, 4)):
            ag[c][q] = remote(
                xbuf.at[pl.ds(s, 4), rows, pl.ds(ext, WB)],
                xbuf.at[pl.ds(4 - s, 4), rows, pl.ds(ext + WB, WB)],
                ags.at[c, q], agv.at[c, q], partner,
            )
            ag[c][q].start()

    def own(c):
        a, b = chunks[c]
        for p in range(max(starts[c], 1), starts[c + 1]):
            exchange[p].wait_recv()
        pick, n0, n1 = picker(c)
        dense = jnp.dot(
            pick, exr[n0 * SLOTS : n1 * SLOTS, :ext], preferred_element_type=F32
        )
        xbuf[0, a:b, :ext] = dense.astype(BF16)
        rows = pl.ds(a, b - a)
        for q, s, cols, device in (
            (0, 3, ag_low, right), (2, 1, ag_high, left),
            (1, 3, ag_high, right), (3, 1, ag_low, left),
        ):
            ag[c][q] = remote(
                xbuf.at[0, rows, cols], xbuf.at[s, rows, cols], ags.at[c, q], agv.at[c, q], device
            )
            ag[c][q].start()
        ag[c][4] = remote(
            xbuf.at[0, rows, ag_all], xbuf.at[4, rows, ag_all], ags.at[c, 4], agv.at[c, 4], partner
        )
        ag[c][4].start()

    def relay(c):
        a, b = chunks[c]
        rows = pl.ds(a, b - a)
        ag[c][5] = remote(
            xbuf.at[3, rows, ag_low], xbuf.at[2, rows, ag_low], ags.at[c, 5], agv.at[c, 5], right
        )
        ag[c][6] = remote(
            xbuf.at[1, rows, ag_high], xbuf.at[2, rows, ag_high], ags.at[c, 6], agv.at[c, 6], left
        )
        ag[c][0].wait_recv()
        ag[c][5].start()
        ag[c][2].wait_recv()
        ag[c][6].start()

    def forward(c):
        a, b = chunks[c]
        rows = pl.ds(a, b - a)
        for q, s, ready in ((7, 3, 1), (8, 1, 3)):
            ag[c][ready].wait_recv()
            ag[c][q] = remote(
                xbuf.at[s, rows, ag_all], xbuf.at[4 + s, rows, ag_all],
                ags.at[c, q], agv.at[c, q], partner,
            )
            ag[c][q].start()

    def far(c):
        a, b = chunks[c]
        rows = pl.ds(a, b - a)
        ag[c][5].wait_recv()
        ag[c][6].wait_recv()
        ag[c][9] = remote(
            xbuf.at[2, rows, ag_all], xbuf.at[6, rows, ag_all], ags.at[c, 9], agv.at[c, 9], partner
        )
        ag[c][9].start()
        for q in (4, 7, 8, 9, 10, 11):
            ag[c][q].wait_recv()

    def gated(c, first, count_tiles):
        a, b = chunks[c]
        span = b - a
        count = 8 * span

        def hidden_tile(i, _):
            contract = (((1,), (1,)), ((), ()))
            acc = lax.dot_general(
                xbuf[:, a:b, :da].reshape(count, da), wgu[i, :, :da], contract,
                preferred_element_type=F32,
            ) + lax.dot_general(
                xbuf[:, a:b, ext:].reshape(count, 2 * WB), wgu[i, :, da:], contract,
                preferred_element_type=F32,
            )
            g, u = acc[:, :LANES], acc[:, LANES:]
            shares = xbuf[:, a:b, da:ext].reshape(count, LANES)

            def hit(e, j):
                at = j + i * LANES - e * hidden
                return (at >= 0) & (at < hidden) & (e < local)

            scale = jnp.dot(
                shares, onehot(LANES, LANES, hit), preferred_element_type=F32
            )
            h = g / (1.0 + jnp.exp(-g)) * u * scale
            hbuf[:count, pl.ds(pl.multiple_of(i * LANES, LANES), LANES)] = h.astype(BF16)
            return _

        lax.fori_loop(first, first + count_tiles, hidden_tile, 0)

    def sent(c):
        for q in range(12):
            ag[c][q].wait_send()

    def down(c, q):
        a, b = chunks[c]
        span = b - a
        count = 8 * span
        tile = 512

        def down_tile(n, _):
            cols = pl.ds(pl.multiple_of(q * half + n * tile, tile), tile)
            out = jnp.dot(hbuf[:count, :], wd[:, cols], preferred_element_type=F32)
            xbuf[:, a:b, cols] = out.astype(BF16).reshape(8, span, tile)
            return _

        lax.fori_loop(0, half // tile, down_tile, 0)
        rows, cols = pl.ds(a, span), (low, high)[q]
        rs[c][q] = remote(
            xbuf.at[pl.ds(4, 4), rows, cols], pr.at[c % 2, :, pl.ds(0, span), cols],
            rss.at[c, q], rsv.at[c, q], partner,
        )
        rs[c][q].start()

    def add(dst, dst_at, srcs, a, b, low, high):
        tile = 512

        def step(n, _):
            cols = pl.ds(pl.multiple_of(low + n * tile, tile), tile)
            total = dst[dst_at, a:b, cols].astype(F32)
            for src in srcs:
                total = total + src(n * tile, tile).astype(F32)
            dst[dst_at, a:b, cols] = total.astype(BF16)
            return _

        lax.fori_loop(0, (high - low) // tile, step, 0)

    def cut(ref, lead, a, b, base):
        def get(at, size):
            cols = pl.ds(pl.multiple_of(base + at, size), size)
            return ref[a:b, cols] if lead is None else ref[lead, a:b, cols]

        return get

    def partner_sum(c, q):
        a, b = chunks[c]
        rows, cols = pl.ds(a, b - a), (low, high)[q]
        at, to = q * half, (q + 1) * half
        rs[c][q].wait_recv()
        far_to, landing = (right, ra) if q == 0 else (left, rb)
        near, near_to, near_at = (3, left, fr) if q == 0 else (1, right, fl)
        add(xbuf, 2, [cut(pr.at[c % 2, 2], None, 0, b - a, at)], a, b, at, to)
        rs[c][2 + q] = remote(
            xbuf.at[2, rows, cols], landing.at[rows], rss.at[c, 2 + q], rsv.at[c, 2 + q], far_to
        )
        rs[c][2 + q].start()
        add(xbuf, near, [cut(pr.at[c % 2, near], None, 0, b - a, at)], a, b, at, to)
        rs[c][4 + q] = remote(
            xbuf.at[near, rows, cols], near_at.at[rows, cols],
            rss.at[c, 4 + q], rsv.at[c, 4 + q], near_to,
        )
        rs[c][4 + q].start()
        add(xbuf, 4 - near, [cut(pr.at[c % 2, 4 - near], None, 0, b - a, at)], a, b, at, to)
        add(xbuf, 0, [cut(pr.at[c % 2, 0], None, 0, b - a, at)], a, b, at, to)

    def ring_sum(c):
        a, b = chunks[c]
        rows = pl.ds(a, b - a)
        for q, s, landed, to, at in ((0, 1, ra, right, fl), (1, 3, rb, left, fr)):
            cols = (low, high)[q]
            rs[c][2 + q].wait_recv()
            add(xbuf, s, [cut(landed, None, a, b, 0)], a, b, q * half, (q + 1) * half)
            rs[c][6 + q] = remote(
                xbuf.at[s, rows, cols], at.at[rows, cols], rss.at[c, 6 + q], rsv.at[c, 6 + q], to
            )
            rs[c][6 + q].start()

    def finish(c):
        a, b = chunks[c]
        for q in (4, 5, 6, 7):
            rs[c][q].wait_recv()
        add(xbuf, 0, [cut(fl, None, a, b, 0), cut(fr, None, a, b, 0)], a, b, 0, width)
        p0 = state["returned"]
        p1 = b // CAP
        state["returned"] = p1
        w0 = p0 * CAP // 16 * 16

        def hit(i, j):
            match = None
            for p in range(p0, p1):
                s = i - (p - p0) * SLOTS
                m = (s >= 0) & (s < CAP) & (j + w0 == s + p * CAP)
                match = m if match is None else match | m
            return match

        spread = onehot((p1 - p0) * SLOTS, b - w0, hit)
        tile = 1280

        def step(n, _):
            cols = pl.ds(pl.multiple_of(n * tile, tile), tile)
            out = jnp.dot(spread, xbuf[0, w0:b, cols], preferred_element_type=F32)
            exr[p0 * SLOTS : p1 * SLOTS, cols] = out.astype(BF16)
            return _

        lax.fori_loop(0, width // tile, step, 0)
        for p in range(p0, p1):
            block = pl.ds(p * SLOTS, SLOTS)
            if p == 0:
                back[:SLOTS, :] = exr[:SLOTS, :width]
            else:
                ret[p] = remote(
                    exr.at[block, pl.ds(0, width)], back.at[block], rts.at[p], rtv.at[p], back_there(p)
                )
                ret[p].start()

    last = len(chunks) - 1
    exchange_rows(0)
    row[0].wait_recv()
    row[2].start()
    row[3].start()
    exchange_rows(1)
    selectors(0)
    row[1].wait_recv()
    row[5].start()
    row[3].wait_recv()
    row[6].start()
    own(0)
    row[2].wait_recv()
    selectors(3)
    row[4].wait_recv()
    selectors(1)
    row[5].wait_recv()
    row[6].wait_recv()
    selectors(2)
    build(0)
    exchange_rows(2)
    build(1)
    relay(0)
    own(1)
    for c in range(3, len(chunks)):
        exchange_rows(c)
    forward(0)
    take(0)
    for w in weights:
        w.wait()
    for c in range(len(chunks)):
        far(c)
        gated(c, 0, 2)
        if c + 1 <= last:
            relay(c + 1)
        if c + 2 <= last:
            own(c + 2)
            build(c + 2)
        gated(c, 2, tiles - 2)
        if c + 1 <= last:
            forward(c + 1)
        if c >= 2:
            finish(c - 2)
        if c >= 1:
            ring_sum(c - 1)
        sent(c)
        down(c, 0)
        down(c, 1)
        partner_sum(c, 0)
        partner_sum(c, 1)
        if c + 1 <= last:
            take(c + 1)
    finish(last - 1)
    ring_sum(last)
    finish(last)
    for q in row:
        q.wait_send()
    for p in range(max(starts[-3], 1), nodes):
        bsend[p].wait_send()
    for p in range(1, nodes):
        exchange[p].wait_send()
    for c in range(len(chunks)):
        for q in range(8):
            rs[c][q].wait_send()
    for p in range(1, nodes):
        ret[p].wait_send()
        ret[p].wait_recv()

    def unpack(n, _):
        cols = pl.ds(pl.multiple_of(n * 1280, 1280), 1280)
        out_ref[:, cols] = jnp.dot(
            spread_rows, back[:, cols], preferred_element_type=F32
        ).astype(BF16)
        return _

    lax.fori_loop(0, width // 1280, unpack, 0)


def shards(tokens, node_ids, expert_pick, gate_share, gate_proj, up_proj, down_proj):
    tok_count, width = tokens.shape
    local, hidden, _ = gate_proj.shape
    nodes = len(HOPS)
    rows = nodes * CAP
    chunks = len(CUTS) - 1
    most = max(b - a for a, b in zip(CUTS[:-1], CUTS[1:]))
    starts = [0] + [(b - 1) // CAP + 1 for b in CUTS[1:]]
    groups = max(b - a for a, b in zip(starts[:-1], starts[1:]))
    tiles = -(-local * hidden // LANES)
    dma = pltpu.SemaphoreType.DMA
    vmem, anywhere = pl.BlockSpec(memory_space=pltpu.VMEM), pl.BlockSpec(memory_space=pl.ANY)
    return pl.pallas_call(
        kernel,
        out_shape=jax.ShapeDtypeStruct((tok_count, width), BF16),
        in_specs=[vmem] * 3 + [anywhere] * 4,
        out_specs=vmem,
        scratch_shapes=[
            pltpu.VMEM((tok_count, width), BF16),
            pltpu.VMEM((nodes * SLOTS, width - 2 * WB + LANES), BF16),
            pltpu.VMEM((4, 2 * tok_count, WB + LANES), BF16),
            pltpu.VMEM((tok_count, WB + LANES), BF16),
            pltpu.VMEM((8, nodes * SLOTS, tok_count), BF16),
            pltpu.VMEM((2, groups, 8, SLOTS, WB), BF16),
            pltpu.VMEM((nodes, 8, SLOTS, WB), BF16),
            pltpu.VMEM((nodes * SLOTS, width), BF16),
            pltpu.VMEM((tiles, 2 * LANES, width), BF16),
            pltpu.VMEM((tiles * LANES, width), BF16),
            pltpu.VMEM((8, rows, width + LANES), BF16),
            pltpu.VMEM((nodes * SLOTS, width), BF16),
            pltpu.VMEM((2, 4, most, width), BF16),
            pltpu.VMEM((rows, width // 2), BF16),
            pltpu.VMEM((rows, width // 2), BF16),
            pltpu.VMEM((rows, width), BF16),
            pltpu.VMEM((rows, width), BF16),
            pltpu.VMEM((8 * most, tiles * LANES), BF16),
            dma((3,)),
            dma((7,)),
            dma((7,)),
            dma((nodes,)),
            dma((nodes,)),
            dma((local * (6 * (hidden // BLOCK) + 1),)),
            dma((nodes,)),
            dma((nodes,)),
            dma((chunks, 12)),
            dma((chunks, 12)),
            dma((chunks, 8)),
            dma((chunks, 8)),
            dma((nodes,)),
            dma((nodes,)),
        ],
        compiler_params=pltpu.CompilerParams(
            collective_id=0, has_side_effects=True, vmem_limit_bytes=67_043_328
        ),
        name="routed_experts",
    )(node_ids, expert_pick, gate_share, tokens, gate_proj, up_proj, down_proj)


def solution(mesh):
    return jax.shard_map(
        shards,
        mesh=mesh,
        in_specs=(
            P(("node", "dev"), None),
            P(("node", "dev"), None),
            P(("node", "dev"), None),
            P(("node", "dev"), None),
            P("node", "dev", None),
            P("node", "dev", None),
            P("node", "dev", None),
        ),
        out_specs=P(("node", "dev"), None),
        check_vma=False,
    )
```
